32 devices in a mesh: row: 8 (over z, core), col: 4 (over y, x).
Axes of the slice: x: 2, y: 2, z: 4, core: 2. Of those that a mesh axis runs over, the one named last changes fastest.
Arguments:
- object_field: float32 [3, 2, 1024, 512], P(None, None, 'row', 'col'), may hold values from -5 to 5
- probe: float32 [2, 128, 128], replicated, may hold values from -5 to 5
- measured: float32 [8, 4, 2, 128, 128], P('row', 'col'), may hold values from 0.25 to 4
- positions: int32 [8, 4, 2, 2], P('row', 'col'), may hold values from 0 to 127
- counts: int32 [8, 4], P('row', 'col'), may hold values from 1 to 2, as said below
Outputs:
- object_next: float32 [3, 2, 1024, 512], P(None, None, 'row', 'col')
The draws below stay inside these ranges and needn't reach their ends.
Inputs may be any that keep to these rules, and one draw needn't show every extreme that they name: Slots 0 to counts - 1 of a tile are live; some tile has all 2 live.
All inputs are finite; a program needn't handle non-finite values.
Results may differ from the reference program's by a relative error of at most 0.0003.
Values sent between devices are 32-bit elements; how exact they have to be, the bound alone decides.
A program may use at most 64 MiB of HBM per device.

```python
import math
import jax
import jax.numpy as jnp
from jax import lax

W = 128
S = 128
SLICES = 3
ITERS = 2
SLOTS = 2
TILE_ROWS = 8
TILE_COLS = 4
ROWS_ALL = 1024
COLS_ALL = 512


def draw_counts(key, part):
    first_key = jax.random.fold_in(key, 11)
    second_key = jax.random.fold_in(key, 12)
    third_key = jax.random.fold_in(key, 13)
    first_draw = jax.random.randint(first_key, (TILE_ROWS, TILE_COLS), 1, SLOTS + 1, dtype=jnp.int32)
    second_draw = jax.random.randint(second_key, (TILE_ROWS, TILE_COLS), 1, SLOTS + 1, dtype=jnp.int32)
    busiest = jax.random.randint(third_key, (), 0, TILE_ROWS * TILE_COLS, dtype=jnp.int32)
    ordinal = jnp.arange(TILE_ROWS * TILE_COLS, dtype=jnp.int32).reshape(TILE_ROWS, TILE_COLS)
    return jnp.where(ordinal == busiest, SLOTS, jnp.minimum(first_draw, second_draw)).astype(jnp.int32)


def place_ends(entries, key, least, high):
    longest = entries.shape.index(max(entries.shape))
    spots = []
    for shift in (0, 1):
        where = [jax.random.randint(jax.random.fold_in(key, axis), (), 0, length) for axis, length in enumerate(entries.shape)]
        where[longest] = (where[longest] + shift) % entries.shape[longest]
        spots.append(tuple(where))
    return entries.at[spots[0]].set(least).at[spots[1]].set(high)


def steps_of(rng, extent, split, low, largest):
    def one(dim, parts):
        steps = jax.random.uniform(jax.random.fold_in(jax.random.fold_in(rng, 6), dim), (parts,), jnp.float32, low / len(split), largest / len(split))
        return jnp.repeat(jnp.exp(steps), extent[dim] // parts).reshape((-1,) + (1,) * (len(extent) - dim - 1))

    factor_of = one(*split[0])
    for cut in split[1:]:
        factor_of = factor_of * one(*cut)
    return factor_of


def centred(stream_key, shape, scale, reach, shards=(), kind=jnp.bfloat16):
    drawn = scale * jax.random.normal(stream_key, shape, jnp.float32)
    if shards:
        drawn = drawn * steps_of(stream_key, shape, shards, -0.22, 0.18)
    return jnp.clip(drawn, -reach, reach).astype(kind)


def setup_inputs(seed: int = 0) -> dict:
    streams_of = jax.random.split(jax.random.key(seed), 6)
    return {
        "object_field": centred(streams_of[0], (SLICES, 2, ROWS_ALL, COLS_ALL), 0.7, 5.0, ((2, 8), (3, 4)), jnp.float32),
        "probe": centred(streams_of[1], (2, W, W), 0.7, 5.0, (), jnp.float32),
        "measured": jnp.clip(jnp.exp(math.log(4.0) - 2.7725887 * jax.random.uniform(streams_of[2], (TILE_ROWS, TILE_COLS, SLOTS, W, W), jnp.float32) ** steps_of(streams_of[2], (TILE_ROWS, TILE_COLS, SLOTS, W, W), ((0, 8), (1, 4)), -0.2, 0.2)), 0.25, 4.0),
        "positions": place_ends(jax.random.randint(streams_of[3], (TILE_ROWS, TILE_COLS, SLOTS, 2), 0, S), jax.random.fold_in(streams_of[3], 1), 0, S - 1).astype(jnp.int32),
        "counts": draw_counts(jax.random.fold_in(streams_of[5], 71), 0),
    }


LEARNING_RATE = 0.02


def phase_table():
    frequency = (jnp.arange(W, dtype=jnp.int32) + W // 2) % W - W // 2
    squares = (frequency[:, None] * frequency[:, None] + frequency[None, :] * frequency[None, :]).astype(jnp.float32)
    angles = (-0.25 * math.pi / W) * squares
    return lax.complex(jnp.cos(angles), jnp.sin(angles))


def propagate(wavefield, kernel):
    return jnp.fft.ifft2(jnp.fft.fft2(wavefield, norm="ortho") * kernel, norm="ortho")


def window_gradient(window, probe_wave, sample, kernel):
    layers = [lax.complex(window[slice_index, 0], window[slice_index, 1]) for slice_index in range(SLICES)]
    wavefield = probe_wave
    incident = []
    for slice_index in range(SLICES):
        incident.append(wavefield)
        wavefield = layers[slice_index] * wavefield
        if slice_index + 1 < SLICES:
            wavefield = propagate(wavefield, kernel)
    far_field = jnp.fft.fft2(wavefield, norm="ortho")
    residue = jnp.real(far_field) ** 2 + jnp.imag(far_field) ** 2 - sample
    back_wave = jnp.fft.ifft2(residue * far_field, norm="ortho")
    pieces = [None] * SLICES
    for slice_index in reversed(range(SLICES)):
        product = jnp.conj(incident[slice_index]) * back_wave
        pieces[slice_index] = jnp.stack([jnp.real(product), jnp.imag(product)])
        if slice_index > 0:
            back_wave = propagate(jnp.conj(layers[slice_index]) * back_wave, jnp.conj(kernel))
    return jnp.stack(pieces)


def reference(object_field, probe, measured, positions, counts):
    rim_width = W // 2
    kernel = phase_table()
    probe_wave = lax.complex(probe[0], probe[1])
    total_windows = TILE_ROWS * TILE_COLS * SLOTS
    flat_corners = positions.reshape(total_windows, 2).astype(jnp.int32)
    flat_samples = measured.reshape(total_windows, W, W)
    ordinal = jnp.arange(total_windows, dtype=jnp.int32)
    tile_number = ordinal // SLOTS
    live_mask = (ordinal % SLOTS < counts.reshape(-1).astype(jnp.int32)[tile_number]).astype(object_field.dtype)
    row_start = ((tile_number // TILE_COLS) * S + flat_corners[:, 0]).astype(jnp.int32)
    col_start = ((tile_number % TILE_COLS) * S + flat_corners[:, 1]).astype(jnp.int32)
    anchor = jnp.zeros((), jnp.int32)
    current = object_field
    for iteration in range(ITERS):
        padded = jnp.pad(current, ((0, 0), (0, 0), (rim_width, rim_width), (rim_width, rim_width)))

        def visit(window_index, running):
            corner_start = (anchor, anchor, row_start[window_index], col_start[window_index])
            window = lax.dynamic_slice(padded, corner_start, (SLICES, 2, W, W))
            update = window_gradient(window, probe_wave, flat_samples[window_index], kernel) * live_mask[window_index]
            before = lax.dynamic_slice(running, corner_start, (SLICES, 2, W, W))
            return lax.dynamic_update_slice(running, before + update.astype(running.dtype), corner_start)

        gradient_sum = lax.fori_loop(0, total_windows, visit, jnp.zeros_like(padded))
        interior = gradient_sum[:, :, rim_width:rim_width + TILE_ROWS * S, rim_width:rim_width + TILE_COLS * S]
        current = current - LEARNING_RATE * interior
    return current
```

```python
import functools

import jax
import jax.numpy as jnp
import ml_dtypes
import numpy as np
from jax import lax
from jax.experimental import pallas as pl
from jax.experimental.pallas import tpu as pltpu
from jax.sharding import PartitionSpec as P

ITERS = 2
LEARNING_RATE = 0.02


def halves_of(matrix):
    block = np.block([[matrix.real, matrix.imag], [-matrix.imag, matrix.real]])
    block = block.astype(np.float32)
    lead = block.astype(ml_dtypes.bfloat16)
    trail = (block - lead.astype(np.float32)).astype(ml_dtypes.bfloat16)
    return np.stack([lead, trail])


def make_tables(side):
    ordinal = np.arange(side)
    fourier = np.exp(-2j * np.pi / side * (np.outer(ordinal, ordinal) % side)) / np.sqrt(side)
    frequency = (ordinal + side // 2) % side - side // 2
    phase = np.exp(-0.25j * np.pi / side * frequency * frequency)
    spread = (fourier.conj() * phase[None, :]) @ fourier
    forms = [fourier, fourier.conj(), spread, spread.conj()]
    return np.stack([halves_of(form) for form in forms])


def split(values):
    lead = values.astype(jnp.bfloat16)
    return lead, (values - lead.astype(jnp.float32)).astype(jnp.bfloat16)


def dot(left, right):
    return jnp.dot(left, right, preferred_element_type=jnp.float32)


def both_sides(waves, table, form):
    side = waves[0][0].shape[0]
    stacked = jnp.concatenate([jnp.concatenate(pair, axis=1) for pair in waves], axis=0)
    lead, trail = split(stacked)
    right = (table[form, 0], table[form, 1])
    out = dot(lead, right[0]) + dot(trail, right[0]) + dot(lead, right[1])
    count = len(waves)
    turned = jnp.concatenate(
        [
            jnp.concatenate(
                [out[w * side : (w + 1) * side, part * side : (part + 1) * side] for w in range(count)],
                axis=1,
            )
            for part in range(2)
        ],
        axis=0,
    )
    lead, trail = split(turned)
    left = (table[form ^ 1, 0], table[form ^ 1, 1])
    out = dot(left[0], lead) + dot(left[0], trail) + dot(left[1], lead)
    return [
        tuple(
            out[part * side : (part + 1) * side, w * side : (w + 1) * side] for part in range(2)
        )
        for w in range(count)
    ]


def times(a, b):
    return (a[0] * b[0] - a[1] * b[1], a[0] * b[1] + a[1] * b[0])


def conj_times(a, b):
    return (a[0] * b[0] + a[1] * b[1], a[0] * b[1] - a[1] * b[0])


def masks_of(corners, window, side):
    half = side // 2
    found = []
    for dim in range(2):
        place = lax.broadcasted_iota(jnp.int32, (side, side), dim)
        corner = corners[window * 2 + dim]
        found.append((place >= corner + half) | (place < corner - half))
    return found


def compute_kernel(tiles, probe, samples, corners, count, table, grads):
    layer_count = tiles.shape[2]
    side = tiles.shape[-1]
    slots = samples.shape[0]
    half = side // 2
    masks = [masks_of(corners, w, side) for w in range(slots)]
    waves = []
    for w in range(slots):
        shifts = [lax.rem(corners[w * 2 + dim] + half, side) for dim in range(2)]
        waves.append(
            tuple(
                pltpu.roll(pltpu.roll(probe[part], shifts[0], 0), shifts[1], 1)
                for part in range(2)
            )
        )

    def layer(w, s):
        rows, cols = masks[w]
        return tuple(
            jnp.where(
                rows,
                jnp.where(cols, tiles[1, 1, s, part], tiles[1, 0, s, part]),
                jnp.where(cols, tiles[0, 1, s, part], tiles[0, 0, s, part]),
            )
            for part in range(2)
        )

    windows = range(slots)
    incident = []
    layers = []
    for s in range(layer_count):
        incident.append(waves)
        layers.append([layer(w, s) for w in windows])
        waves = [times(layers[s][w], waves[w]) for w in windows]
        if s + 1 < layer_count:
            waves = both_sides(waves, table, 2)
    far = both_sides(waves, table, 0)
    scaled = []
    for w in windows:
        residue = far[w][0] * far[w][0] + far[w][1] * far[w][1] - samples[w]
        scaled.append((residue * far[w][0], residue * far[w][1]))
    back = both_sides(scaled, table, 1)
    for s in reversed(range(layer_count)):
        pieces = [conj_times(incident[s][w], back[w]) for w in windows]
        for part in range(2):
            totals = [[0.0, 0.0], [0.0, 0.0]]
            for w in windows:
                rows, cols = masks[w]
                value = jnp.where(w < count[0], pieces[w][part], 0.0)
                split_rows = (jnp.where(rows, 0.0, value), jnp.where(rows, value, 0.0))
                for a in range(2):
                    totals[a][0] += jnp.where(cols, 0.0, split_rows[a])
                    totals[a][1] += jnp.where(cols, split_rows[a], 0.0)
            for a in range(2):
                for b in range(2):
                    grads[a, b, s, part] = totals[a][b]
        if s > 0:
            back = both_sides(
                [conj_times(layers[s][w], back[w]) for w in windows], table, 3
            )


def shifted(block, axis, step):
    size = lax.axis_size(axis)
    route = [(i, i + step) for i in range(size) if 0 <= i + step < size]
    return lax.ppermute(block, axis, route)


def swapped(block, axis, dim, outward):
    half = block.shape[dim] // 2
    low = lax.slice_in_dim(block, 0, half, axis=dim)
    high = lax.slice_in_dim(block, half, None, axis=dim)
    return jnp.concatenate([shifted(low, axis, outward), shifted(high, axis, -outward)], axis=dim)


def shards(object_field, probe, measured, positions, counts):
    samples = measured[0, 0]
    corners = positions[0, 0].reshape(-1)
    count = counts.reshape(-1)
    table = jnp.asarray(make_tables(probe.shape[-1]))
    vmem = pl.BlockSpec(memory_space=pltpu.VMEM)
    smem = pl.BlockSpec(memory_space=pltpu.SMEM)
    current = object_field
    compute = pl.pallas_call(
        compute_kernel,
        out_shape=jax.ShapeDtypeStruct((2, 2) + object_field.shape, jnp.float32),
        in_specs=[vmem, vmem, vmem, smem, smem, vmem],
        out_specs=vmem,
        name="windows",
    )
    for _ in range(ITERS):
        wide = jnp.stack([current, swapped(current, "col", 3, -1)])
        tiles = jnp.stack([wide, swapped(wide, "row", 3, -1)])
        grads = compute(tiles, probe, samples, corners, count, table)
        folded = grads[0] + swapped(grads[1], "row", 3, 1)
        current = current - LEARNING_RATE * (folded[0] + swapped(folded[1], "col", 3, 1))
    return current


def solution(mesh):
    placed = (
        P(None, None, "row", "col"),
        P(),
        P("row", "col", None, None, None),
        P("row", "col", None, None),
        P("row", "col"),
    )
    return jax.shard_map(
        shards, mesh=mesh, in_specs=placed, out_specs=P(None, None, "row", "col"), check_vma=False
    )
```

```python
import functools

import jax
import jax.numpy as jnp
import ml_dtypes
import numpy as np
from jax import lax
from jax.experimental import pallas as pl
from jax.experimental.pallas import tpu as pltpu
from jax.sharding import PartitionSpec as P

ITERS = 2
LEARNING_RATE = 0.02


def halves_of(matrix):
    block = np.block([[matrix.real, matrix.imag], [-matrix.imag, matrix.real]])
    block = block.astype(np.float32)
    lead = block.astype(ml_dtypes.bfloat16)
    trail = (block - lead.astype(np.float32)).astype(ml_dtypes.bfloat16)
    return np.stack([lead, trail])


def make_tables(side):
    ordinal = np.arange(side)
    fourier = np.exp(-2j * np.pi / side * (np.outer(ordinal, ordinal) % side)) / np.sqrt(side)
    frequency = (ordinal + side // 2) % side - side // 2
    phase = np.exp(-0.25j * np.pi / side * frequency * frequency)
    spread = (fourier.conj() * phase[None, :]) @ fourier
    forms = [fourier, fourier.conj(), spread, spread.conj()]
    return np.stack([halves_of(form) for form in forms])


def split(values):
    lead = values.astype(jnp.bfloat16)
    return lead, (values - lead.astype(jnp.float32)).astype(jnp.bfloat16)


def dot(left, right):
    return jnp.dot(left, right, preferred_element_type=jnp.float32)


def both_sides(waves, table, form):
    side = waves[0][0].shape[0]
    stacked = jnp.concatenate([jnp.concatenate(pair, axis=1) for pair in waves], axis=0)
    lead, trail = split(stacked)
    right = (table[form, 0], table[form, 1])
    out = dot(lead, right[0]) + dot(trail, right[0]) + dot(lead, right[1])
    count = len(waves)
    turned = jnp.concatenate(
        [
            jnp.concatenate(
                [out[w * side : (w + 1) * side, part * side : (part + 1) * side] for w in range(count)],
                axis=1,
            )
            for part in range(2)
        ],
        axis=0,
    )
    lead, trail = split(turned)
    left = (table[form ^ 1, 0], table[form ^ 1, 1])
    out = dot(left[0], lead) + dot(left[0], trail) + dot(left[1], lead)
    return [
        tuple(
            out[part * side : (part + 1) * side, w * side : (w + 1) * side] for part in range(2)
        )
        for w in range(count)
    ]


def times(a, b):
    return (a[0] * b[0] - a[1] * b[1], a[0] * b[1] + a[1] * b[0])


def conj_times(a, b):
    return (a[0] * b[0] + a[1] * b[1], a[0] * b[1] - a[1] * b[0])


def masks_of(corners, window, side):
    half = side // 2
    found = []
    for dim in range(2):
        place = lax.broadcasted_iota(jnp.int32, (side, side), dim)
        corner = corners[window * 2 + dim]
        found.append((place >= corner + half) | (place < corner - half))
    return found


def pack(tile):
    half = tile.shape[0] // 2
    lane = lax.broadcasted_iota(jnp.int32, (half, tile.shape[1]), 1)
    low, high = tile[:half], tile[half:]
    left = jnp.where(lane < half, low, pltpu.roll(high, half, 1))
    right = jnp.where(lane < half, pltpu.roll(low, half, 1), high)
    return left, right


def unpack(left, right):
    half = left.shape[0]
    lane = lax.broadcasted_iota(jnp.int32, left.shape, 1)
    low = jnp.where(lane < half, left, pltpu.roll(right, half, 1))
    high = jnp.where(lane < half, pltpu.roll(left, half, 1), right)
    return jnp.concatenate([low, high], axis=0)


PHASES = ("tall", "wide", "corner", "fold_rows", "fold_cols")


def step_kernel(
    shape, field, probe, samples, corners, count, table_far, out,
    table, later, vert, horz, diag, halo_out, halo_in, grad_rows, grad_in, grad_cols, fold_in,
    kept, send_sem, recv_sem, table_sem,
):
    layer_count = field.shape[0]
    side = field.shape[-1]
    slots = samples.shape[0]
    half = side // 2
    windows = range(slots)
    slices = range(layer_count)
    me = {axis: lax.axis_index(axis) for axis in shape}
    has = {axis: (me[axis] > 0, me[axis] < shape[axis] - 1) for axis in shape}
    own = [field] + [later.at[t] for t in range(ITERS - 1)]
    parts = (pl.ds(0, half), pl.ds(half, half))

    def copy(phase, t, s, d):
        if phase == "tall":
            axis, src, dst = "row", own[t].at[s, :, parts[d]], vert.at[t, s, :, parts[d]]
        elif phase == "wide":
            axis, src, dst = "col", halo_out.at[t, d, s], halo_in.at[t, d, s]
        elif phase == "corner":
            axis, src, dst = "row", horz.at[t, s, :, parts[d]], diag.at[t, s, :, parts[d]]
        elif phase == "fold_rows":
            rows = parts[1 - d]
            axis, src, dst = "row", grad_rows.at[t, s, :, :, rows], grad_in.at[t, s, :, :, rows]
        else:
            axis, src, dst = "col", grad_cols.at[t, 1 - d, s], fold_in.at[t, 1 - d, s]
        number = PHASES.index(phase)
        return axis, dst, pltpu.make_async_remote_copy(
            src_ref=src,
            dst_ref=dst,
            send_sem=send_sem.at[t, number, s, d],
            recv_sem=recv_sem.at[t, number, s, d],
            device_id={axis: me[axis] + (1 if d else -1)},
            device_id_type=pl.DeviceIdType.MESH,
        )

    def start(phase, t, s):
        for d in range(2):
            axis, _, moved = copy(phase, t, s, d)
            pl.when(has[axis][d])(moved.start)

    def arrive(phase, t, s):
        for d in range(2):
            axis, _, moved = copy(phase, t, s, d)
            pl.when(has[axis][1 - d])(moved.wait_recv)

    def uses():
        for t in range(ITERS):
            for phase in PHASES:
                for s in slices:
                    for d in range(2):
                        yield copy(phase, t, s, d) + (d,)

    load = pltpu.make_async_copy(table_far, table, table_sem)
    load.start()
    barrier = pltpu.get_barrier_semaphore()
    for axis in shape:
        for d in range(2):

            @pl.when(has[axis][d])
            def greet():
                pl.semaphore_signal(
                    barrier,
                    inc=1,
                    device_id={axis: me[axis] + (1 if d else -1)},
                    device_id_type=pl.DeviceIdType.MESH,
                )

    def ship_wide(t, s):
        for part in range(2):
            for d, piece in enumerate(pack(own[t][s, part])):
                halo_out[t, d, s, part] = piece
        start("wide", t, s)

    def ship_corner(t, s):
        arrive("wide", t, s)
        for part in range(2):
            horz[t, s, part] = unpack(halo_in[t, 0, s, part], halo_in[t, 1, s, part])
        start("corner", t, s)

    peers = sum(there.astype(jnp.int32) for axis in shape for there in has[axis])
    pl.semaphore_wait(barrier, peers)
    for s in slices:
        start("tall", 0, s)
        ship_wide(0, s)
    for axis, dst, _, d in uses():

        @pl.when(jnp.logical_not(has[axis][1 - d]))
        def clear():
            dst[...] = jnp.zeros(dst.shape, jnp.float32)

    masks = [masks_of(corners, w, side) for w in windows]
    beams = []
    for w in windows:
        shifts = [lax.rem(corners[w * 2 + dim] + half, side) for dim in range(2)]
        beams.append(
            tuple(
                pltpu.roll(pltpu.roll(probe[part], shifts[0], 0), shifts[1], 1)
                for part in range(2)
            )
        )
    load.wait()

    def layer(t, s, w):
        rows, cols = masks[w]
        return tuple(
            jnp.where(
                rows,
                jnp.where(cols, diag[t, s, part], vert[t, s, part]),
                jnp.where(cols, horz[t, s, part], own[t][s, part]),
            )
            for part in range(2)
        )

    def gather_grads(t, s, pieces):
        for part in range(2):
            totals = [[0.0, 0.0], [0.0, 0.0]]
            for w in windows:
                rows, cols = masks[w]
                value = jnp.where(w < count[0], pieces[w][part], 0.0)
                by_rows = (jnp.where(rows, 0.0, value), jnp.where(rows, value, 0.0))
                for a in range(2):
                    totals[a][0] += jnp.where(cols, 0.0, by_rows[a])
                    totals[a][1] += jnp.where(cols, by_rows[a], 0.0)
            for b in range(2):
                kept[b, s, part] = totals[0][b]
                grad_rows[t, s, b, part] = totals[1][b]
        start("fold_rows", t, s)

    def ship_cols(t, s):
        arrive("fold_rows", t, s)
        for part in range(2):
            aside = kept[1, s, part] + grad_in[t, s, 1, part]
            for d, piece in enumerate(pack(aside)):
                grad_cols[t, d, s, part] = piece
        start("fold_cols", t, s)

    def update(t, s, target):
        arrive("fold_cols", t, s)
        for part in range(2):
            inner = kept[0, s, part] + grad_in[t, s, 0, part]
            total = inner + unpack(fold_in[t, 0, s, part], fold_in[t, 1, s, part])
            target[s, part] = own[t][s, part] - LEARNING_RATE * total

    for t in range(ITERS):
        if t > 0:
            for s in slices:
                start("tall", t, s)
                ship_wide(t, s)
        waves = beams
        incident, layers = [], []
        ship_corner(t, 0)
        for s in slices:
            if s + 1 < layer_count:
                ship_corner(t, s + 1)
            arrive("tall", t, s)
            arrive("corner", t, s)
            incident.append(waves)
            layers.append([layer(t, s, w) for w in windows])
            waves = [times(layers[s][w], waves[w]) for w in windows]
            if s + 1 < layer_count:
                waves = both_sides(waves, table, 2)
        far = both_sides(waves, table, 0)
        scaled = []
        for w in windows:
            residue = far[w][0] * far[w][0] + far[w][1] * far[w][1] - samples[w]
            scaled.append((residue * far[w][0], residue * far[w][1]))
        back = both_sides(scaled, table, 1)
        for s in reversed(slices):
            gather_grads(t, s, [conj_times(incident[s][w], back[w]) for w in windows])
            if s + 1 < layer_count:
                ship_cols(t, s + 1)
            if s > 0:
                back = both_sides(
                    [conj_times(layers[s][w], back[w]) for w in windows], table, 3
                )
        ship_cols(t, 0)
        for s in reversed(slices):
            update(t, s, out if t + 1 == ITERS else own[t + 1])
    for axis, _, moved, d in uses():
        pl.when(has[axis][d])(moved.wait_send)


def shards(shape, object_field, probe, measured, positions, counts):
    samples = measured[0, 0]
    corners = positions[0, 0].reshape(-1)
    count = counts.reshape(-1)
    tables = make_tables(probe.shape[-1])
    vmem = pl.BlockSpec(memory_space=pltpu.VMEM)
    smem = pl.BlockSpec(memory_space=pltpu.SMEM)
    layer_count, _, side, _ = object_field.shape
    tiles = (layer_count, 2, side, side)
    packed = (ITERS, 2, layer_count, 2, side // 2, side)
    shapes = [
        (ITERS - 1,) + tiles,
        (ITERS,) + tiles,
        (ITERS,) + tiles,
        (ITERS,) + tiles,
        packed,
        packed,
        (ITERS, layer_count, 2, 2, side, side),
        (ITERS, layer_count, 2, 2, side, side),
        packed,
        packed,
        (2,) + tiles,
    ]
    sems = (ITERS, len(PHASES), layer_count, 2)
    return pl.pallas_call(
        functools.partial(step_kernel, shape),
        out_shape=jax.ShapeDtypeStruct(object_field.shape, jnp.float32),
        in_specs=[vmem, vmem, vmem, smem, smem, pl.BlockSpec(memory_space=pltpu.HBM)],
        out_specs=vmem,
        scratch_shapes=[pltpu.VMEM(tables.shape, jnp.bfloat16)]
        + [pltpu.VMEM(size, jnp.float32) for size in shapes]
        + [
            pltpu.SemaphoreType.DMA(sems),
            pltpu.SemaphoreType.DMA(sems),
            pltpu.SemaphoreType.DMA,
        ],
        compiler_params=pltpu.CompilerParams(collective_id=0, has_side_effects=True),
        name="steps",
    )(object_field, probe, samples, corners, count, jnp.asarray(tables))


def solution(mesh):
    placed = (
        P(None, None, "row", "col"),
        P(),
        P("row", "col", None, None, None),
        P("row", "col", None, None),
        P("row", "col"),
    )
    return jax.shard_map(
        functools.partial(shards, dict(mesh.shape)),
        mesh=mesh,
        in_specs=placed,
        out_specs=P(None, None, "row", "col"),
        check_vma=False,
    )
```

```python
import functools

import jax
import jax.numpy as jnp
import ml_dtypes
import numpy as np
from jax import lax
from jax.experimental import pallas as pl
from jax.experimental.pallas import tpu as pltpu
from jax.sharding import PartitionSpec as P

ITERS = 2
LEARNING_RATE = 0.02


def halves_of(matrix):
    block = np.block([[matrix.real, matrix.imag], [-matrix.imag, matrix.real]])
    block = block.astype(np.float32)
    lead = block.astype(ml_dtypes.bfloat16)
    trail = (block - lead.astype(np.float32)).astype(ml_dtypes.bfloat16)
    return np.stack([lead, trail])


def make_tables(side):
    ordinal = np.arange(side)
    fourier = np.exp(-2j * np.pi / side * (np.outer(ordinal, ordinal) % side)) / np.sqrt(side)
    frequency = (ordinal + side // 2) % side - side // 2
    phase = np.exp(-0.25j * np.pi / side * frequency * frequency)
    spread = (fourier.conj() * phase[None, :]) @ fourier
    forms = [fourier, fourier.conj(), spread, spread.conj()]
    return np.stack([halves_of(form) for form in forms])


def split(values):
    lead = values.astype(jnp.bfloat16)
    return lead, (values - lead.astype(jnp.float32)).astype(jnp.bfloat16)


def dot(left, right):
    return jnp.dot(left, right, preferred_element_type=jnp.float32)


def both_sides(waves, table, form):
    side = waves[0][0].shape[0]
    stacked = jnp.concatenate([jnp.concatenate(pair, axis=1) for pair in waves], axis=0)
    lead, trail = split(stacked)
    right = (table[form, 0], table[form, 1])
    out = dot(lead, right[0]) + dot(trail, right[0]) + dot(lead, right[1])
    count = len(waves)
    turned = jnp.concatenate(
        [
            jnp.concatenate(
                [out[w * side : (w + 1) * side, part * side : (part + 1) * side] for w in range(count)],
                axis=1,
            )
            for part in range(2)
        ],
        axis=0,
    )
    lead, trail = split(turned)
    left = (table[form ^ 1, 0], table[form ^ 1, 1])
    out = dot(left[0], lead) + dot(left[0], trail) + dot(left[1], lead)
    return [
        tuple(
            out[part * side : (part + 1) * side, w * side : (w + 1) * side] for part in range(2)
        )
        for w in range(count)
    ]


def times(a, b):
    return (a[0] * b[0] - a[1] * b[1], a[0] * b[1] + a[1] * b[0])


def conj_times(a, b):
    return (a[0] * b[0] + a[1] * b[1], a[0] * b[1] - a[1] * b[0])


def masks_of(corners, window, side):
    half = side // 2
    found = []
    for dim in range(2):
        place = lax.broadcasted_iota(jnp.int32, (side, side), dim)
        corner = corners[0, 0, window, dim]
        found.append((place >= corner + half) | (place < corner - half))
    return found


def pack(tile):
    half = tile.shape[0] // 2
    lane = lax.broadcasted_iota(jnp.int32, (half, tile.shape[1]), 1)
    low, high = tile[:half], tile[half:]
    left = jnp.where(lane < half, low, pltpu.roll(high, half, 1))
    right = jnp.where(lane < half, pltpu.roll(low, half, 1), high)
    return left, right


def unpack(left, right):
    half = left.shape[0]
    lane = lax.broadcasted_iota(jnp.int32, left.shape, 1)
    low = jnp.where(lane < half, left, pltpu.roll(right, half, 1))
    high = jnp.where(lane < half, pltpu.roll(left, half, 1), right)
    return jnp.concatenate([low, high], axis=0)


PHASES = ("tall", "wide0", "wide1", "corner", "fold_rows", "fold_cols0", "fold_cols1")
RELAYED = ("wide1", "fold_cols1")


def step_kernel(
    shape, field, probe, samples, corners, count, table_far, out,
    table, later, vert, horz, diag, halo_out, halo_in, grad_rows, grad_in, grad_cols, fold_in,
    kept, relay, relay_send, relay_recv, pass_send, send_sem, recv_sem, table_sem,
):
    layer_count = field.shape[0]
    side = field.shape[-1]
    slots = samples.shape[0]
    half = side // 2
    windows = range(slots)
    slices = range(layer_count)
    me = {axis: lax.axis_index(axis) for axis in shape}
    has = {axis: (me[axis] > 0, me[axis] < shape[axis] - 1) for axis in shape}
    own = [field] + [later.at[t] for t in range(ITERS - 1)]
    parts = (pl.ds(0, half), pl.ds(half, half))
    detour = shape["col"] == 4

    def turns(phase, d):
        return (me["col"] == 2 - d) if detour and phase in RELAYED else None

    def both(here, phase, d):
        away = turns(phase, d)
        return here if away is None else jnp.logical_and(here, jnp.logical_not(away))

    def copy(phase, t, s, d, leg=0):
        if phase == "tall":
            axis, src, dst = "row", own[t].at[s, :, parts[d]], vert.at[t, s, :, parts[d]]
        elif phase.startswith("wide"):
            part = int(phase[-1])
            axis, src, dst = "col", halo_out.at[t, d, s, part], halo_in.at[t, d, s, part]
        elif phase == "corner":
            axis, src, dst = "row", horz.at[t, s, :, parts[d]], diag.at[t, s, :, parts[d]]
        elif phase == "fold_rows":
            rows = parts[1 - d]
            axis, src, dst = "row", grad_rows.at[t, s, :, :, rows], grad_in.at[t, s, :, :, rows]
        else:
            part = int(phase[-1])
            axis, src = "col", grad_cols.at[t, 1 - d, s, part]
            dst = fold_in.at[t, 1 - d, s, part]
        number = PHASES.index(phase)
        step = 1 if d else -1

        def moved(src, dst, sent, landed, step):
            return pltpu.make_async_remote_copy(
                src_ref=src,
                dst_ref=dst,
                send_sem=sent,
                recv_sem=landed,
                device_id={axis: me[axis] + step},
                device_id_type=pl.DeviceIdType.MESH,
            )

        landed = recv_sem.at[t, number, s, d]
        if leg == 0:
            return axis, dst, moved(src, dst, send_sem.at[t, number, s, d], landed, step)
        slot = (t, RELAYED.index(phase), s)
        if leg == 1:
            held = relay.at[slot]
            return axis, held, moved(src, held, relay_send.at[slot], relay_recv.at[slot], 2 * step)
        return axis, dst, moved(relay.at[slot], dst, pass_send.at[slot], landed, -step)

    def start(phase, t, s):
        for d in range(2):
            axis, _, moved = copy(phase, t, s, d)
            pl.when(both(has[axis][d], phase, d))(moved.start)
            if turns(phase, d) is not None:
                pl.when(turns(phase, d))(copy(phase, t, s, d, 1)[2].start)

    def hand_on(phase, t, s):
        for d in range(2):
            if turns(phase, d) is not None:

                @pl.when(me["col"] == (3 if d else 0))
                def forward():
                    copy(phase, t, s, d, 1)[2].wait_recv()
                    copy(phase, t, s, d, 2)[2].start()

    def arrive(phase, t, s):
        for d in range(2):
            axis, _, moved = copy(phase, t, s, d)
            pl.when(has[axis][1 - d])(moved.wait_recv)

    def uses():
        for t in range(ITERS):
            for phase in PHASES:
                for s in slices:
                    for d in range(2):
                        yield copy(phase, t, s, d) + (phase, d)

    load = pltpu.make_async_copy(table_far, table, table_sem)
    load.start()
    barrier = pltpu.get_barrier_semaphore()
    for axis in shape:
        for d in range(2):

            @pl.when(has[axis][d])
            def greet():
                pl.semaphore_signal(
                    barrier,
                    inc=1,
                    device_id={axis: me[axis] + (1 if d else -1)},
                    device_id_type=pl.DeviceIdType.MESH,
                )

    if detour:
        pl.semaphore_signal(
            barrier,
            inc=1,
            device_id={"col": lax.rem(me["col"] + 2, shape["col"])},
            device_id_type=pl.DeviceIdType.MESH,
        )

    def ship_wide(t, s):
        for part in range(2):
            for d, piece in enumerate(pack(own[t][s, part])):
                halo_out[t, d, s, part] = piece
        start("wide1", t, s)
        start("wide0", t, s)

    def ship_corner(t, s):
        arrive("wide0", t, s)
        arrive("wide1", t, s)
        for part in range(2):
            horz[t, s, part] = unpack(halo_in[t, 0, s, part], halo_in[t, 1, s, part])
        start("corner", t, s)

    peers = sum(there.astype(jnp.int32) for axis in shape for there in has[axis])
    pl.semaphore_wait(barrier, peers + (1 if detour else 0))
    for s in slices:
        start("tall", 0, s)
        ship_wide(0, s)
        if s > 0:
            hand_on("wide1", 0, s - 1)
    hand_on("wide1", 0, layer_count - 1)
    for axis, dst, _, _, d in uses():

        @pl.when(jnp.logical_not(has[axis][1 - d]))
        def clear():
            dst[...] = jnp.zeros(dst.shape, jnp.float32)

    masks = [masks_of(corners, w, side) for w in windows]
    beams = []
    for w in windows:
        shifts = [lax.rem(corners[0, 0, w, dim] + half, side) for dim in range(2)]
        beams.append(
            tuple(
                pltpu.roll(pltpu.roll(probe[part], shifts[0], 0), shifts[1], 1)
                for part in range(2)
            )
        )
    load.wait()

    def layer(t, s, w):
        rows, cols = masks[w]
        return tuple(
            jnp.where(
                rows,
                jnp.where(cols, diag[t, s, part], vert[t, s, part]),
                jnp.where(cols, horz[t, s, part], own[t][s, part]),
            )
            for part in range(2)
        )

    def gather_grads(t, s, pieces):
        for part in range(2):
            totals = [[0.0, 0.0], [0.0, 0.0]]
            for w in windows:
                rows, cols = masks[w]
                value = jnp.where(w < count[0, 0], pieces[w][part], 0.0)
                by_rows = (jnp.where(rows, 0.0, value), jnp.where(rows, value, 0.0))
                for a in range(2):
                    totals[a][0] += jnp.where(cols, 0.0, by_rows[a])
                    totals[a][1] += jnp.where(cols, by_rows[a], 0.0)
            for b in range(2):
                kept[b, s, part] = totals[0][b]
                grad_rows[t, s, b, part] = totals[1][b]
        start("fold_rows", t, s)

    def ship_cols(t, s):
        arrive("fold_rows", t, s)
        for part in range(2):
            aside = kept[1, s, part] + grad_in[t, s, 1, part]
            for d, piece in enumerate(pack(aside)):
                grad_cols[t, d, s, part] = piece
        start("fold_cols1", t, s)
        start("fold_cols0", t, s)

    def update(t, s, target):
        arrive("fold_cols0", t, s)
        arrive("fold_cols1", t, s)
        for part in range(2):
            inner = kept[0, s, part] + grad_in[t, s, 0, part]
            total = inner + unpack(fold_in[t, 0, s, part], fold_in[t, 1, s, part])
            target[s, part] = own[t][s, part] - LEARNING_RATE * total

    for t in range(ITERS):
        if t > 0:
            for s in slices:
                start("tall", t, s)
                ship_wide(t, s)
                if s > 0:
                    hand_on("wide1", t, s - 1)
            hand_on("wide1", t, layer_count - 1)
        waves = beams
        incident, layers = [], []
        ship_corner(t, 0)
        for s in slices:
            if s + 1 < layer_count:
                ship_corner(t, s + 1)
            arrive("tall", t, s)
            arrive("corner", t, s)
            incident.append(waves)
            layers.append([layer(t, s, w) for w in windows])
            waves = [times(layers[s][w], waves[w]) for w in windows]
            if s + 1 < layer_count:
                waves = both_sides(waves, table, 2)
        far = both_sides(waves, table, 0)
        scaled = []
        for w in windows:
            residue = far[w][0] * far[w][0] + far[w][1] * far[w][1] - samples[w]
            scaled.append((residue * far[w][0], residue * far[w][1]))
        back = both_sides(scaled, table, 1)
        for s in reversed(slices):
            gather_grads(t, s, [conj_times(incident[s][w], back[w]) for w in windows])
            if s + 1 < layer_count:
                ship_cols(t, s + 1)
            if s + 2 < layer_count:
                hand_on("fold_cols1", t, s + 2)
            if s > 0:
                back = both_sides(
                    [conj_times(layers[s][w], back[w]) for w in windows], table, 3
                )
        ship_cols(t, 0)
        for s in reversed(range(min(2, layer_count))):
            hand_on("fold_cols1", t, s)
        for s in reversed(slices):
            update(t, s, out if t + 1 == ITERS else own[t + 1])
    for axis, _, moved, phase, d in uses():
        pl.when(both(has[axis][d], phase, d))(moved.wait_send)
    for t in range(ITERS):
        for phase in RELAYED:
            for s in slices:
                for d in range(2):
                    if turns(phase, d) is not None:
                        pl.when(turns(phase, d))(copy(phase, t, s, d, 1)[2].wait_send)
                        pl.when(me["col"] == (3 if d else 0))(copy(phase, t, s, d, 2)[2].wait_send)


def shards(shape, object_field, probe, measured, positions, counts):
    samples = measured[0, 0]
    tables = make_tables(probe.shape[-1])
    vmem = pl.BlockSpec(memory_space=pltpu.VMEM)
    smem = pl.BlockSpec(memory_space=pltpu.SMEM)
    layer_count, _, side, _ = object_field.shape
    tiles = (layer_count, 2, side, side)
    packed = (ITERS, 2, layer_count, 2, side // 2, side)
    shapes = [
        (ITERS - 1,) + tiles,
        (ITERS,) + tiles,
        (ITERS,) + tiles,
        (ITERS,) + tiles,
        packed,
        packed,
        (ITERS, layer_count, 2, 2, side, side),
        (ITERS, layer_count, 2, 2, side, side),
        packed,
        packed,
        (2,) + tiles,
        (ITERS, len(RELAYED), layer_count, side // 2, side),
    ]
    relays = pltpu.SemaphoreType.DMA((ITERS, len(RELAYED), layer_count))
    sems = (ITERS, len(PHASES), layer_count, 2)
    return pl.pallas_call(
        functools.partial(step_kernel, shape),
        out_shape=jax.ShapeDtypeStruct(object_field.shape, jnp.float32),
        in_specs=[vmem, vmem, vmem, smem, smem, pl.BlockSpec(memory_space=pltpu.HBM)],
        out_specs=vmem,
        scratch_shapes=[pltpu.VMEM(tables.shape, jnp.bfloat16)]
        + [pltpu.VMEM(size, jnp.float32) for size in shapes]
        + [
            relays,
            relays,
            relays,
            pltpu.SemaphoreType.DMA(sems),
            pltpu.SemaphoreType.DMA(sems),
            pltpu.SemaphoreType.DMA,
        ],
        compiler_params=pltpu.CompilerParams(collective_id=0, has_side_effects=True),
        name="steps",
    )(object_field, probe, samples, positions, counts, jnp.asarray(tables))


def solution(mesh):
    placed = (
        P(None, None, "row", "col"),
        P(),
        P("row", "col", None, None, None),
        P("row", "col", None, None),
        P("row", "col"),
    )
    return jax.shard_map(
        functools.partial(shards, dict(mesh.shape)),
        mesh=mesh,
        in_specs=placed,
        out_specs=P(None, None, "row", "col"),
        check_vma=False,
    )
```
